32 devices in a mesh: batch: 8 (over y, x, core), cols: 4 (over z).
Axes of the slice: x: 2, y: 2, z: 4, core: 2. Of those that a mesh axis runs over, the one named last changes fastest.
Arguments:
- grad_up: float32 [8, 1024, 4096], P('batch', None, 'cols'), may hold values from -0.875 to 0.875
- grad_down: float32 [8, 4096, 1024], P('batch', 'cols'), may hold values from -0.875 to 0.875
- grad_query: float32 [8, 1024, 1024], P('batch', None, 'cols'), may hold values from -0.875 to 0.875
- grad_key: float32 [8, 1024, 1024], P('batch', None, 'cols'), may hold values from -0.875 to 0.875
- grad_value: float32 [8, 1024, 1024], P('batch', None, 'cols'), may hold values from -0.875 to 0.875
- grad_mixed: float32 [8, 1024, 1024], P('batch', 'cols'), may hold values from -0.875 to 0.875
- grad_norm: float32 [8, 1024], P('batch'), may hold values from -8 to 8
- weight_up: float32 [1024, 4096], P('batch', 'cols'), may hold values from -0.1875 to 0.1875
- weight_down: float32 [4096, 1024], P('cols', 'batch'), may hold values from -0.09375 to 0.09375
- weight_query: float32 [1024, 1024], P('batch', 'cols'), may hold values from -0.1875 to 0.1875
- weight_key: float32 [1024, 1024], P('batch', 'cols'), may hold values from -0.1875 to 0.1875
- weight_value: float32 [1024, 1024], P('batch', 'cols'), may hold values from -0.1875 to 0.1875
- weight_mixed: float32 [1024, 1024], P('cols', 'batch'), may hold values from -0.1875 to 0.1875
- weight_norm: float32 [1024], P('batch'), may hold values from 0.25 to 1.75
- moment_up: float32 [1024, 4096], P('batch', 'cols'), may hold values from -1.75 to 1.75
- moment_down: float32 [4096, 1024], P('cols', 'batch'), may hold values from -1.75 to 1.75
- moment_query: float32 [1024, 1024], P('batch', 'cols'), may hold values from -1.75 to 1.75
- moment_key: float32 [1024, 1024], P('batch', 'cols'), may hold values from -1.75 to 1.75
- moment_value: float32 [1024, 1024], P('batch', 'cols'), may hold values from -1.75 to 1.75
- moment_mixed: float32 [1024, 1024], P('cols', 'batch'), may hold values from -1.75 to 1.75
- moment_norm: float32 [1024], P('batch'), may hold values from -1.75 to 1.75
Outputs:
- copy_up: bfloat16 [1024, 4096], P(None, 'cols')
- copy_down: bfloat16 [4096, 1024], P('cols')
- copy_query: bfloat16 [1024, 1024], P(None, 'cols')
- copy_key: bfloat16 [1024, 1024], P(None, 'cols')
- copy_value: bfloat16 [1024, 1024], P(None, 'cols')
- copy_mixed: bfloat16 [1024, 1024], P('cols')
- copy_norm: bfloat16 [1024], replicated
- new_up: float32 [1024, 4096], P('batch', 'cols')
- new_down: float32 [4096, 1024], P('cols', 'batch')
- new_query: float32 [1024, 1024], P('batch', 'cols')
- new_key: float32 [1024, 1024], P('batch', 'cols')
- new_value: float32 [1024, 1024], P('batch', 'cols')
- new_mixed: float32 [1024, 1024], P('cols', 'batch')
- new_norm: float32 [1024], P('batch')
- state_new_up: float32 [1024, 4096], P('batch', 'cols')
- state_new_down: float32 [4096, 1024], P('cols', 'batch')
- state_new_query: float32 [1024, 1024], P('batch', 'cols')
- state_new_key: float32 [1024, 1024], P('batch', 'cols')
- state_new_value: float32 [1024, 1024], P('batch', 'cols')
- state_new_mixed: float32 [1024, 1024], P('cols', 'batch')
- state_new_norm: float32 [1024], P('batch')
The draws below stay inside these ranges and needn't reach their ends.
All inputs are finite; a program needn't handle non-finite values.
Results may differ from the reference program's by a relative error of at most 0.008.
Values may be sent and summed in bfloat16 or wider, within the bound.
A program may use at most 64 MiB of HBM per device.

```python
import jax
import jax.numpy as jnp

WIDTH = 1024
INNER = 4096
ATTN = 1024
REPLICAS = 8


def spiked(entries, rng, source, target, blocks, factor):
    owner, partner = [(jnp.arange(entries.shape[dim]) // (entries.shape[dim] // blocks)).reshape([-1 if axis == dim else 1 for axis in range(entries.ndim)]) for dim in (source, target)]
    chosen = jax.random.permutation(rng, blocks)[partner]
    strong = (owner == chosen) | (owner == (partner + blocks // 2) % blocks)
    return jnp.where(strong, factor * entries, entries)


def steps_of(rng, dims, cuts, smallest, top_value):
    level = 1.0
    for dim, parts in cuts:
        heights = jax.random.uniform(jax.random.fold_in(jax.random.fold_in(rng, 6), dim), (parts,), jnp.float32, smallest / len(cuts), top_value / len(cuts))
        level = level * jnp.repeat(jnp.exp(heights), dims[dim] // parts).reshape((-1,) + (1,) * (len(dims) - 1 - dim))
    return level


def centred(key, shape, scale, bound, pieces=(), kind=jnp.bfloat16):
    loudness = steps_of(key, shape, pieces, -0.22, 0.18) if pieces else 1.0
    drawn = jax.random.normal(key, shape, jnp.float32) * scale * loudness
    return jnp.minimum(jnp.maximum(drawn, -bound), bound).astype(kind)


def bell_draw_with(own_key, shape, deviation, most, split, heavy, kind=jnp.bfloat16):
    array = deviation * jax.random.normal(own_key, shape, jnp.float32)
    if split:
        array = array * steps_of(own_key, shape, split, -0.22, 0.18)
    return jnp.clip(spiked(array, jax.random.fold_in(own_key, 3), *heavy), -most, most).astype(kind)


def setup_inputs(seed: int = 0) -> dict:
    arg_keys = jax.random.split(jax.random.key(seed), 22)
    return {
        "grad_up": bell_draw_with(arg_keys[0], (REPLICAS, WIDTH, INNER), 0.1, 0.875, ((0, 8), (2, 4)), (0, 1, 8, 2.0), jnp.float32),
        "grad_down": bell_draw_with(arg_keys[1], (REPLICAS, INNER, WIDTH), 0.1, 0.875, ((0, 8), (1, 4)), (0, 2, 8, 2.0), jnp.float32),
        "grad_query": bell_draw_with(arg_keys[2], (REPLICAS, WIDTH, ATTN), 0.1, 0.875, ((0, 8), (2, 4)), (0, 1, 8, 2.0), jnp.float32),
        "grad_key": bell_draw_with(arg_keys[3], (REPLICAS, WIDTH, ATTN), 0.1, 0.875, ((0, 8), (2, 4)), (0, 1, 8, 2.0), jnp.float32),
        "grad_value": bell_draw_with(arg_keys[4], (REPLICAS, WIDTH, ATTN), 0.1, 0.875, ((0, 8), (2, 4)), (0, 1, 8, 2.0), jnp.float32),
        "grad_mixed": bell_draw_with(arg_keys[5], (REPLICAS, ATTN, WIDTH), 0.1, 0.875, ((0, 8), (1, 4)), (0, 2, 8, 2.0), jnp.float32),
        "grad_norm": bell_draw_with(arg_keys[6], (REPLICAS, WIDTH), 1.0, 8.0, ((0, 8),), (0, 1, 8, 2.0), jnp.float32),
        "weight_up": centred(arg_keys[7], (WIDTH, INNER), WIDTH ** -0.5, 0.1875, ((0, 8), (1, 4)), jnp.float32),
        "weight_down": centred(arg_keys[8], (INNER, WIDTH), INNER ** -0.5, 0.09375, ((0, 4), (1, 8)), jnp.float32),
        "weight_query": centred(arg_keys[9], (WIDTH, ATTN), WIDTH ** -0.5, 0.1875, ((0, 8), (1, 4)), jnp.float32),
        "weight_key": centred(arg_keys[10], (WIDTH, ATTN), WIDTH ** -0.5, 0.1875, ((0, 8), (1, 4)), jnp.float32),
        "weight_value": centred(arg_keys[11], (WIDTH, ATTN), WIDTH ** -0.5, 0.1875, ((0, 8), (1, 4)), jnp.float32),
        "weight_mixed": centred(arg_keys[12], (ATTN, WIDTH), ATTN ** -0.5, 0.1875, ((0, 4), (1, 8)), jnp.float32),
        "weight_norm": jnp.clip(1.0 + 0.15 * jax.random.normal(arg_keys[13], (WIDTH,), jnp.float32), 0.25, 1.75),
        "moment_up": centred(arg_keys[14], (WIDTH, INNER), 0.3, 1.75, ((0, 8), (1, 4)), jnp.float32),
        "moment_down": centred(arg_keys[15], (INNER, WIDTH), 0.3, 1.75, ((0, 4), (1, 8)), jnp.float32),
        "moment_query": centred(arg_keys[16], (WIDTH, ATTN), 0.3, 1.75, ((0, 8), (1, 4)), jnp.float32),
        "moment_key": centred(arg_keys[17], (WIDTH, ATTN), 0.3, 1.75, ((0, 8), (1, 4)), jnp.float32),
        "moment_value": centred(arg_keys[18], (WIDTH, ATTN), 0.3, 1.75, ((0, 8), (1, 4)), jnp.float32),
        "moment_mixed": centred(arg_keys[19], (ATTN, WIDTH), 0.3, 1.75, ((0, 4), (1, 8)), jnp.float32),
        "moment_norm": centred(arg_keys[20], (WIDTH,), 0.3, 1.75, ((0, 8),), jnp.float32),
    }


learn_rate = 0.1
hold_rate = 0.7


def reference(grad_up, grad_down, grad_query, grad_key, grad_value, grad_mixed, grad_norm, weight_up, weight_down, weight_query, weight_key, weight_value, weight_mixed, weight_norm, moment_up, moment_down, moment_query, moment_key, moment_value, moment_mixed, moment_norm):
    mean_up = jnp.sum(grad_up.astype(jnp.float32), axis=0) * REPLICAS ** -0.5
    mean_down = jnp.sum(grad_down.astype(jnp.float32), axis=0) * REPLICAS ** -0.5
    mean_query = jnp.sum(grad_query.astype(jnp.float32), axis=0) * REPLICAS ** -0.5
    mean_key = jnp.sum(grad_key.astype(jnp.float32), axis=0) * REPLICAS ** -0.5
    mean_value = jnp.sum(grad_value.astype(jnp.float32), axis=0) * REPLICAS ** -0.5
    mean_mixed = jnp.sum(grad_mixed.astype(jnp.float32), axis=0) * REPLICAS ** -0.5
    mean_norm = jnp.sum(grad_norm.astype(jnp.float32), axis=0) * REPLICAS ** -0.5
    state_new_up = hold_rate * moment_up + mean_up
    new_up = weight_up - learn_rate * state_new_up
    state_new_down = hold_rate * moment_down + mean_down
    new_down = weight_down - learn_rate * state_new_down
    state_new_query = hold_rate * moment_query + mean_query
    new_query = weight_query - learn_rate * state_new_query
    state_new_key = hold_rate * moment_key + mean_key
    new_key = weight_key - learn_rate * state_new_key
    state_new_value = hold_rate * moment_value + mean_value
    new_value = weight_value - learn_rate * state_new_value
    state_new_mixed = hold_rate * moment_mixed + mean_mixed
    new_mixed = weight_mixed - learn_rate * state_new_mixed
    state_new_norm = hold_rate * moment_norm + mean_norm
    new_norm = weight_norm - learn_rate * state_new_norm
    copy_up = new_up.astype(jnp.bfloat16)
    copy_down = new_down.astype(jnp.bfloat16)
    copy_query = new_query.astype(jnp.bfloat16)
    copy_key = new_key.astype(jnp.bfloat16)
    copy_value = new_value.astype(jnp.bfloat16)
    copy_mixed = new_mixed.astype(jnp.bfloat16)
    copy_norm = new_norm.astype(jnp.bfloat16)
    return copy_up, copy_down, copy_query, copy_key, copy_value, copy_mixed, copy_norm, new_up, new_down, new_query, new_key, new_value, new_mixed, new_norm, state_new_up, state_new_down, state_new_query, state_new_key, state_new_value, state_new_mixed, state_new_norm
```

```python
import functools

import jax
import jax.numpy as jnp
from jax import lax
from jax.experimental import pallas as pl
from jax.experimental.pallas import tpu as pltpu
from jax.sharding import PartitionSpec as P

learn_rate = 0.1
hold_rate = 0.7


def body(
    grad_up,
    grad_down,
    grad_query,
    grad_key,
    grad_value,
    grad_mixed,
    grad_norm,
    weight_up,
    weight_down,
    weight_query,
    weight_key,
    weight_value,
    weight_mixed,
    weight_norm,
    moment_up,
    moment_down,
    moment_query,
    moment_key,
    moment_value,
    moment_mixed,
    moment_norm,
):
    mean_up, mean_down, mean_query, mean_key, mean_value, mean_mixed = (
        lax.psum_scatter(
            grad_up[0].astype(jnp.bfloat16), "batch", scatter_dimension=0, tiled=True
        ).astype(jnp.float32),
        lax.psum_scatter(
            grad_down[0].astype(jnp.bfloat16), "batch", scatter_dimension=1, tiled=True
        ).astype(jnp.float32),
        lax.psum_scatter(
            grad_query[0].astype(jnp.bfloat16), "batch", scatter_dimension=0, tiled=True
        ).astype(jnp.float32),
        lax.psum_scatter(
            grad_key[0].astype(jnp.bfloat16), "batch", scatter_dimension=0, tiled=True
        ).astype(jnp.float32),
        lax.psum_scatter(
            grad_value[0].astype(jnp.bfloat16), "batch", scatter_dimension=0, tiled=True
        ).astype(jnp.float32),
        lax.psum_scatter(
            grad_mixed[0].astype(jnp.bfloat16), "batch", scatter_dimension=1, tiled=True
        ).astype(jnp.float32),
    )
    whole_norm = lax.psum(grad_norm[0], "batch")
    place = lax.axis_index("batch")
    mean_norm = lax.dynamic_slice_in_dim(
        whole_norm, place * weight_norm.shape[0], weight_norm.shape[0]
    )
    mean_rate = lax.axis_size("batch") ** (-0.5)
    mean_up = mean_up * mean_rate
    mean_down = mean_down * mean_rate
    mean_query = mean_query * mean_rate
    mean_key = mean_key * mean_rate
    mean_value = mean_value * mean_rate
    mean_mixed = mean_mixed * mean_rate
    mean_norm = mean_norm * mean_rate
    state_new_up = hold_rate * moment_up + mean_up
    new_up = weight_up - learn_rate * state_new_up
    state_new_down = hold_rate * moment_down + mean_down
    new_down = weight_down - learn_rate * state_new_down
    state_new_query = hold_rate * moment_query + mean_query
    new_query = weight_query - learn_rate * state_new_query
    state_new_key = hold_rate * moment_key + mean_key
    new_key = weight_key - learn_rate * state_new_key
    state_new_value = hold_rate * moment_value + mean_value
    new_value = weight_value - learn_rate * state_new_value
    state_new_mixed = hold_rate * moment_mixed + mean_mixed
    new_mixed = weight_mixed - learn_rate * state_new_mixed
    state_new_norm = hold_rate * moment_norm + mean_norm
    new_norm = weight_norm - learn_rate * state_new_norm
    copy_up, copy_down, copy_query, copy_key, copy_value, copy_mixed, copy_norm = (
        lax.all_gather(new_up.astype(jnp.bfloat16), "batch", axis=0, tiled=True),
        lax.all_gather(new_down.astype(jnp.bfloat16), "batch", axis=1, tiled=True),
        lax.all_gather(new_query.astype(jnp.bfloat16), "batch", axis=0, tiled=True),
        lax.all_gather(new_key.astype(jnp.bfloat16), "batch", axis=0, tiled=True),
        lax.all_gather(new_value.astype(jnp.bfloat16), "batch", axis=0, tiled=True),
        lax.all_gather(new_mixed.astype(jnp.bfloat16), "batch", axis=1, tiled=True),
        lax.all_gather(new_norm.astype(jnp.bfloat16), "batch", axis=0, tiled=True),
    )
    return (
        copy_up,
        copy_down,
        copy_query,
        copy_key,
        copy_value,
        copy_mixed,
        copy_norm,
        new_up,
        new_down,
        new_query,
        new_key,
        new_value,
        new_mixed,
        new_norm,
        state_new_up,
        state_new_down,
        state_new_query,
        state_new_key,
        state_new_value,
        state_new_mixed,
        state_new_norm,
    )


PLANS = (((2, (1, 1)), (0, (1, 1)), (3, (1, 1))), ((4, (1,1)), (1, (1, 1)), (5, (1, 1))))
AHEAD = 1
BY_ROWS = (True, False, True, True, True, False)
LOAD, SEND, RECV, KINDS = 0, 1, 7, 13


def pieces_of(shapes):
    lists = []
    for s, plan in enumerate(PLANS):
        lists.append([])
        for m, shares in plan:
            row = 0
            for share in shares:
                rows = shapes[m][0] * share // sum(shares)
                lists[s].append((2 * len(lists[s]) + s, m, row, rows, s == 0))
                row += rows
    return lists


def exchange(shapes, n, *refs):
    refs = list(refs)

    def take(count):
        out, refs[:] = refs[:count], refs[count:]
        return out

    lists = pieces_of(shapes)
    pairs = len(lists[0])
    grads, weights, moments = take(6), take(6), take(6)
    norm_inputs = take(3)
    gathered, news, states = take(6), take(6), take(6)
    norm_copy, norm_new, norm_state = take(3)
    grad_v, weight_v, moment_v = (take(6) for _ in range(3))
    send_1, recv_1, send_2, recv_2, keep_2 = (take(2 * pairs) for _ in range(5))
    send_3, recv_3, keep_3 = (take(2 * pairs) for _ in range(3))
    norm_held = take(3)
    norm_send, norm_recv, norm_full = take(3)
    sems, param_sems, norm_sems, norm_load_sems = take(4)

    me = lax.axis_index("batch")
    c = lax.rem(me, 2)
    x = lax.rem(lax.div(me, 2), 2)
    y = lax.div(me, 4)
    other_c, other_x, other_y = me + 1 - 2 * c, me + 2 - 4 * x, me + 4 - 8 * y
    rate = n ** (-0.5)

    barrier = pltpu.get_barrier_semaphore()
    for device in (other_c, other_x, other_y):
        pl.semaphore_signal(
            barrier, inc=1, device_id={"batch": device}, device_id_type=pl.DeviceIdType.MESH
        )

    def load(piece):
        i, m, row, rows, _ = piece
        at = pl.ds(row, rows)
        if BY_ROWS[m]:
            source, target = grads[m].at[:, at, :], grad_v[m].at[:, at, :]
        else:
            source, target = grads[m].at[at, :], grad_v[m].at[at, :]
        return pltpu.make_async_copy(source, target, sems.at[i, LOAD])

    def params(m):
        return (
            pltpu.make_async_copy(weights[m], weight_v[m], param_sems.at[m, 0]),
            pltpu.make_async_copy(moments[m], moment_v[m], param_sems.at[m, 1]),
        )

    def remote(source, target, send_sem, recv_sem, device):
        return pltpu.make_async_remote_copy(
            src_ref=source,
            dst_ref=target,
            send_sem=send_sem,
            recv_sem=recv_sem,
            device_id={"batch": device},
            device_id_type=pl.DeviceIdType.MESH,
        )

    def hop(piece, step):
        i, m, row, rows, x_first = piece
        first, second = (other_x, other_y) if x_first else (other_y, other_x)
        at = pl.ds(row, rows)
        place = gathered[m]
        if step == 0:
            source, target, device = send_1[i], recv_1[i], other_c
        elif step == 1:
            source, target, device = send_2[i], recv_2[i], first
        elif step == 2:
            source, target, device = send_3[i], recv_3[i], second
        else:
            if step == 3:
                part, device = place.at[y, x, c, at, :], second
            elif step == 4:
                part = place.at[:, x, c, at, :] if x_first else place.at[y, :, c, at, :]
                device = first
            else:
                part, device = place.at[:, :, c, at, :], other_c
            source = target = part
        return remote(source, target, sems.at[i, SEND + step], sems.at[i, RECV + step], device)

    def block(piece, owner):
        _, m, row, rows, _ = piece
        at = pl.ds(row, rows)
        if BY_ROWS[m]:
            return grad_v[m][owner, at, :]
        width = shapes[m][1]
        return grad_v[m][at, pl.ds(pl.multiple_of(owner * width, width), width)]

    waited = set()

    def stage(piece, step):
        i, m, row, rows, x_first = piece
        f, s = (x, y) if x_first else (y, x)
        at = pl.ds(row, rows)

        def spot(first, second):
            return 2 * second + first if x_first else 2 * first + second

        if step == 0:
            load(piece).wait()
            for q in range(4):
                send_1[i][q] = block(piece, 2 * q + 1 - c).astype(jnp.bfloat16)
            hop(piece, 0).start()
        elif step == 1:
            hop(piece, 0).wait_recv()
            for second in range(2):
                q = spot(1 - f, second)
                total = block(piece, 2 * q + c) + recv_1[i][q].astype(jnp.float32)
                send_2[i][second] = total.astype(jnp.bfloat16)
            hop(piece, 1).start()
            for second in range(2):
                q = spot(f, second)
                keep_2[i][second] = block(piece, 2 * q + c) + recv_1[i][q].astype(jnp.float32)
        elif step == 2:
            hop(piece, 1).wait_recv()
            total = keep_2[i][1 - s] + recv_2[i][1 - s].astype(jnp.float32)
            send_3[i][...] = total.astype(jnp.bfloat16)
            hop(piece, 2).start()
            keep_3[i][...] = keep_2[i][s] + recv_2[i][s].astype(jnp.float32)
            hop(piece, 0).wait_send()
        elif step == 3:
            if m not in waited:
                waited.add(m)
                for copy in params(m):
                    copy.wait()
            hop(piece, 2).wait_recv()
            mean = (keep_3[i][...] + recv_3[i][...].astype(jnp.float32)) * rate
            state = hold_rate * moment_v[m][at, :] + mean
            new = weight_v[m][at, :] - learn_rate * state
            gathered[m][y, x, c, at, :] = new.astype(jnp.bfloat16)
            hop(piece, 3).start()
            news[m][at, :] = new
            states[m][at, :] = state
            hop(piece, 1).wait_send()
        elif step == 4:
            hop(piece, 3).wait_recv()
            hop(piece, 4).start()
            hop(piece, 2).wait_send()
        elif step == 5:
            hop(piece, 4).wait_recv()
            hop(piece, 5).start()
            hop(piece, 3).wait_send()
        else:
            hop(piece, 5).wait_recv()
            hop(piece, 4).wait_send()
            hop(piece, 5).wait_send()

    def both(step, p):
        for s in range(2):
            stage(lists[s][p], step)

    def norm_loads():
        return [
            pltpu.make_async_copy(source, target, norm_load_sems.at[i])
            for i, (source, target) in enumerate(zip(norm_inputs, norm_held))
        ]

    def norm_hop(step):
        device = (other_c, other_x, other_y)[step]
        return remote(
            norm_send.at[step], norm_recv.at[step], norm_sems.at[0, step], norm_sems.at[1, step], device
        )

    def norm_stage(step):
        width = norm_held[1].shape[1]
        if step == 0:
            for copy in norm_loads():
                copy.wait()
            for j in range(n):
                norm_send[0, 0, pl.ds(j, 1), :] = norm_held[0][:, j * width : (j + 1) * width]
            own = lax.broadcasted_iota(jnp.int32, (n, width), 0) == me
            for j in (1, 2):
                norm_send[0, j] = jnp.where(own, jnp.broadcast_to(norm_held[j][...], (n, width)), 0.0)
            norm_hop(0).start()
            return
        norm_hop(step - 1).wait_recv()
        total = norm_send[step - 1] + norm_recv[step - 1]
        if step < 3:
            norm_send[step] = total
            norm_hop(step).start()
            return
        state = hold_rate * total[2] + total[0] * rate
        new = total[1] - learn_rate * state
        norm_copy[...] = new.astype(jnp.bfloat16)
        norm_full[0] = new
        norm_full[1] = state
        norm_new[...] = norm_full[0, pl.ds(me, 1), :]
        norm_state[...] = norm_full[1, pl.ds(me, 1), :]
        for i in range(3):
            norm_hop(i).wait_send()

    for p in range(pairs):
        for s in range(2):
            load(lists[s][p]).start()
        if p == AHEAD:
            for copy in norm_loads():
                copy.start()
    for m in dict.fromkeys(m for pair in zip(*PLANS) for m, _ in pair):
        for copy in params(m):
            copy.start()
    pl.semaphore_wait(barrier, 3)

    for p in range(pairs + AHEAD):
        if p < pairs:
            both(0, p)
        if p >= AHEAD:
            both(1, p - AHEAD)
        if p == AHEAD + 1:
            norm_stage(0)
    norm_stage(1)
    for p in range(pairs):
        both(2, p)
    norm_stage(2)
    for p in range(pairs):
        both(3, p)
    norm_stage(3)
    for step in (4, 5, 6):
        for p in range(pairs):
            both(step, p)


def write_out(shapes, n, *refs):
    refs = list(refs)

    def take(count):
        out, refs[:] = refs[:count], refs[count:]
        return out

    gathered, plain_in = take(6), take(15)
    copies, plain_out = take(6), take(15)
    (sems,) = take(1)
    moves = []
    for m in range(6):
        if BY_ROWS[m]:
            moves.append((gathered[m], copies[m]))
            continue
        width = shapes[m][1]
        for j in range(n):
            source = gathered[m].at[j // 4, j // 2 % 2, j % 2]
            moves.append((source, copies[m].at[:, pl.ds(j * width, width)]))
    moves += zip(plain_in, plain_out)
    started = [pltpu.make_async_copy(a, b, sems.at[i]) for i, (a, b) in enumerate(moves)]
    for copy in started:
        copy.start()
    for copy in started:
        copy.wait()


def kernel_body(*args):
    n = lax.axis_size("batch")
    grads, grad_norm = [a[0] for a in args[:6]], args[6]
    weights, weight_norm = args[7:13], args[13]
    moments, moment_norm = args[14:20], args[20]
    shapes = [w.shape for w in weights]
    grads = [g.reshape((n, *s)) if by_rows else g for g, s, by_rows in zip(grads, shapes, BY_ROWS)]
    width = weight_norm.shape[0]
    bf16, f32 = jnp.bfloat16, jnp.float32
    any_spec = pl.BlockSpec(memory_space=pl.ANY)
    vmem_spec = pl.BlockSpec(memory_space=pltpu.VMEM)
    hbm_spec = pl.BlockSpec(memory_space=pltpu.HBM)
    lists = pieces_of(shapes)
    assert len(lists[0]) == len(lists[1])
    ordered = [piece for pair in zip(*lists) for piece in pair]

    def scratch(lead, kind):
        return [pltpu.VMEM((*lead, rows, shapes[m][1]), kind) for _, m, _, rows, _ in ordered]

    whole = [pltpu.VMEM(s, f32) for s in shapes]
    plain = [jax.ShapeDtypeStruct(s, f32) for s in shapes] * 2 + [
        jax.ShapeDtypeStruct((n, width), bf16),
        jax.ShapeDtypeStruct((1, width), f32),
        jax.ShapeDtypeStruct((1, width), f32),
    ]
    parts = [jax.ShapeDtypeStruct((2, 2, 2, *s), bf16) for s in shapes]
    norms = (grad_norm, weight_norm.reshape(1, width), moment_norm.reshape(1, width))
    arrays = (*grads, *weights, *moments, *norms)
    results = pl.pallas_call(
        functools.partial(exchange, shapes, n),
        out_shape=parts + plain,
        in_specs=[any_spec] * 21,
        out_specs=[vmem_spec] * 21,
        scratch_shapes=[pltpu.VMEM(g.shape, f32) for g in grads]
        + whole * 2
        + scratch((4,), bf16) * 2
        + scratch((2,), bf16) * 2
        + scratch((2,), f32)
        + scratch((), bf16) * 2
        + scratch((), f32)
        + [pltpu.VMEM((1, n * width), f32)]
        + [pltpu.VMEM((1, width), f32)] * 2
        + [pltpu.VMEM((3, 3, n, width), f32)] * 2
        + [pltpu.VMEM((2, n, width), f32)]
        + [
            pltpu.SemaphoreType.DMA((len(ordered), KINDS)),
            pltpu.SemaphoreType.DMA((6, 2)),
            pltpu.SemaphoreType.DMA((2, 3)),
            pltpu.SemaphoreType.DMA((3,)),
        ],
        compiler_params=pltpu.CompilerParams(
            collective_id=0, has_side_effects=True, vmem_limit_bytes=40 * 2**20
        ),
    )(*[pltpu.with_memory_space_constraint(a, pltpu.HBM) for a in arrays])
    columns = sum(not by_rows for by_rows in BY_ROWS)
    finals = pl.pallas_call(
        functools.partial(write_out, shapes, n),
        out_shape=[
            part if by_rows else jax.ShapeDtypeStruct((s[0], n * s[1]), bf16)
            for part, s, by_rows in zip(parts, shapes, BY_ROWS)
        ]
        + plain,
        in_specs=[any_spec] * 21,
        out_specs=[hbm_spec] * 21,
        scratch_shapes=[pltpu.SemaphoreType.DMA((21 + columns * (n - 1),))],
        compiler_params=pltpu.CompilerParams(vmem_limit_bytes=8 * 2**20),
    )(*[pltpu.with_memory_space_constraint(r, pltpu.VMEM) for r in results])
    copy = [f.reshape(-1, f.shape[-1]) for f in finals[:6]]
    new, state = finals[6:12], finals[12:18]
    copy_norm, new_norm, state_norm = (r.reshape(-1) for r in finals[18:])
    return (*copy, copy_norm, *new, new_norm, *state, state_norm)


def chosen(*args):
    fits = lax.axis_size("batch") == 2**3 and args[13].shape[0] % 128 == 0
    for m, shares in PLANS[0] + PLANS[1]:
        w = args[7 + m]
        fits = fits and w.shape[0] % (16 * sum(shares)) == 0 and w.shape[1] % 128 == 0
    return kernel_body(*args) if fits else body(*args)


def solution(mesh):
    in_specs = (
        P("batch", None, "cols"),
        P("batch", "cols", None),
        P("batch", None, "cols"),
        P("batch", None, "cols"),
        P("batch", None, "cols"),
        P("batch", "cols", None),
        P("batch", None),
        P("batch", "cols"),
        P("cols", "batch"),
        P("batch", "cols"),
        P("batch", "cols"),
        P("batch", "cols"),
        P("cols", "batch"),
        P("batch"),
        P("batch", "cols"),
        P("cols", "batch"),
        P("batch", "cols"),
        P("batch", "cols"),
        P("batch", "cols"),
        P("cols", "batch"),
        P("batch"),
    )
    out_specs = (
        P(None, "cols"),
        P("cols", None),
        P(None, "cols"),
        P(None, "cols"),
        P(None, "cols"),
        P("cols", None),
        P(),
        P("batch", "cols"),
        P("cols", "batch"),
        P("batch", "cols"),
        P("batch", "cols"),
        P("batch", "cols"),
        P("cols", "batch"),
        P("batch"),
        P("batch", "cols"),
        P("cols", "batch"),
        P("batch", "cols"),
        P("batch", "cols"),
        P("batch", "cols"),
        P("cols", "batch"),
        P("batch"),
    )
    return jax.shard_map(chosen, mesh=mesh, in_specs=in_specs, out_specs=out_specs, check_vma=False)
```

```python
import functools

import jax
import jax.numpy as jnp
from jax import lax
from jax.experimental import pallas as pl
from jax.experimental.pallas import tpu as pltpu
from jax.sharding import PartitionSpec as P

learn_rate = 0.1
hold_rate = 0.7


def body(
    grad_up,
    grad_down,
    grad_query,
    grad_key,
    grad_value,
    grad_mixed,
    grad_norm,
    weight_up,
    weight_down,
    weight_query,
    weight_key,
    weight_value,
    weight_mixed,
    weight_norm,
    moment_up,
    moment_down,
    moment_query,
    moment_key,
    moment_value,
    moment_mixed,
    moment_norm,
):
    mean_up, mean_down, mean_query, mean_key, mean_value, mean_mixed = (
        lax.psum_scatter(
            grad_up[0].astype(jnp.bfloat16), "batch", scatter_dimension=0, tiled=True
        ).astype(jnp.float32),
        lax.psum_scatter(
            grad_down[0].astype(jnp.bfloat16), "batch", scatter_dimension=1, tiled=True
        ).astype(jnp.float32),
        lax.psum_scatter(
            grad_query[0].astype(jnp.bfloat16), "batch", scatter_dimension=0, tiled=True
        ).astype(jnp.float32),
        lax.psum_scatter(
            grad_key[0].astype(jnp.bfloat16), "batch", scatter_dimension=0, tiled=True
        ).astype(jnp.float32),
        lax.psum_scatter(
            grad_value[0].astype(jnp.bfloat16), "batch", scatter_dimension=0, tiled=True
        ).astype(jnp.float32),
        lax.psum_scatter(
            grad_mixed[0].astype(jnp.bfloat16), "batch", scatter_dimension=1, tiled=True
        ).astype(jnp.float32),
    )
    whole_norm = lax.psum(grad_norm[0], "batch")
    place = lax.axis_index("batch")
    mean_norm = lax.dynamic_slice_in_dim(
        whole_norm, place * weight_norm.shape[0], weight_norm.shape[0]
    )
    mean_rate = lax.axis_size("batch") ** (-0.5)
    mean_up = mean_up * mean_rate
    mean_down = mean_down * mean_rate
    mean_query = mean_query * mean_rate
    mean_key = mean_key * mean_rate
    mean_value = mean_value * mean_rate
    mean_mixed = mean_mixed * mean_rate
    mean_norm = mean_norm * mean_rate
    state_new_up = hold_rate * moment_up + mean_up
    new_up = weight_up - learn_rate * state_new_up
    state_new_down = hold_rate * moment_down + mean_down
    new_down = weight_down - learn_rate * state_new_down
    state_new_query = hold_rate * moment_query + mean_query
    new_query = weight_query - learn_rate * state_new_query
    state_new_key = hold_rate * moment_key + mean_key
    new_key = weight_key - learn_rate * state_new_key
    state_new_value = hold_rate * moment_value + mean_value
    new_value = weight_value - learn_rate * state_new_value
    state_new_mixed = hold_rate * moment_mixed + mean_mixed
    new_mixed = weight_mixed - learn_rate * state_new_mixed
    state_new_norm = hold_rate * moment_norm + mean_norm
    new_norm = weight_norm - learn_rate * state_new_norm
    copy_up, copy_down, copy_query, copy_key, copy_value, copy_mixed, copy_norm = (
        lax.all_gather(new_up.astype(jnp.bfloat16), "batch", axis=0, tiled=True),
        lax.all_gather(new_down.astype(jnp.bfloat16), "batch", axis=1, tiled=True),
        lax.all_gather(new_query.astype(jnp.bfloat16), "batch", axis=0, tiled=True),
        lax.all_gather(new_key.astype(jnp.bfloat16), "batch", axis=0, tiled=True),
        lax.all_gather(new_value.astype(jnp.bfloat16), "batch", axis=0, tiled=True),
        lax.all_gather(new_mixed.astype(jnp.bfloat16), "batch", axis=1, tiled=True),
        lax.all_gather(new_norm.astype(jnp.bfloat16), "batch", axis=0, tiled=True),
    )
    return (
        copy_up,
        copy_down,
        copy_query,
        copy_key,
        copy_value,
        copy_mixed,
        copy_norm,
        new_up,
        new_down,
        new_query,
        new_key,
        new_value,
        new_mixed,
        new_norm,
        state_new_up,
        state_new_down,
        state_new_query,
        state_new_key,
        state_new_value,
        state_new_mixed,
        state_new_norm,
    )


PLANS = (
    ((2, ((1, 3),)), (0, ((1, 1), (2,))), (3, ((1, 1),))),
    ((4, ((1, 3),)), (1, ((1, 1), (2,))), (5, ((1, 1),))),
)
LEAD = 2
BY_ROWS = (True, False, True, True, True, False)
LOAD, CORE, FIRST, KINDS = 0, 1, 2, 3


def pieces_of(shapes):
    lists = []
    count = 0
    for s, plan in enumerate(PLANS):
        lists.append([])
        for m, shares in plan:
            row = 0
            unit = shapes[m][0] // sum(map(sum, shares))
            for group in shares:
                start, pieces = row, []
                for share in group:
                    pieces.append((count, m, row, unit * share, s == 0))
                    row += unit * share
                    count += 1
                lists[s].append((2 * len(lists[s]) + s, m, start, row - start, s == 0, pieces))
    return lists


def exchange(shapes, n, *refs):
    refs = list(refs)

    def take(count):
        out, refs[:] = refs[:count], refs[count:]
        return out

    lists = pieces_of(shapes)
    groups = len(lists[0])
    streams = [[piece for group in groups_s for piece in group[-1]] for groups_s in lists]
    pairs = len(streams[0])
    early = [piece[0] for pair in zip(*streams) for piece in pair]
    grads, weights, moments = take(6), take(6), take(6)
    norm_inputs = take(3)
    gathered, news, states = take(6), take(6), take(6)
    norm_copy, norm_new, norm_state = take(3)
    grad_v, param_v = take(6), take(6)
    send_1, recv_1, send_2, recv_2, keep_2 = (take(2 * pairs) for _ in range(5))
    send_3, recv_3, keep_3 = (take(2 * groups) for _ in range(3))
    norm_held = take(3)
    norm_send, norm_recv, norm_full = take(3)
    sems, send_sems, group_sems, norm_sems = take(4)

    me = lax.axis_index("batch")
    c = lax.rem(me, 2)
    x = lax.rem(lax.div(me, 2), 2)
    y = lax.div(me, 4)
    other_c, other_x, other_y = me + 1 - 2 * c, me + 2 - 4 * x, me + 4 - 8 * y
    rate = n ** (-0.5)

    barrier = pltpu.get_barrier_semaphore()
    for device in (other_c, other_x, other_y):
        pl.semaphore_signal(
            barrier, inc=1, device_id={"batch": device}, device_id_type=pl.DeviceIdType.MESH
        )

    def load(piece):
        i, m, row, rows, _ = piece
        at = pl.ds(row, rows)
        if BY_ROWS[m]:
            source, target = grads[m].at[:, at, :], grad_v[m].at[:, at, :]
        else:
            source, target = grads[m].at[at, :], grad_v[m].at[at, :]
        return pltpu.make_async_copy(source, target, sems.at[i, LOAD])

    def params(m):
        sem = sems.at[early[m], LOAD]
        return (
            pltpu.make_async_copy(weights[m], param_v[m].at[0], sem),
            pltpu.make_async_copy(moments[m], param_v[m].at[1], sem),
        )

    def params_wait(m):
        pltpu.make_async_copy(param_v[m], param_v[m], sems.at[early[m], LOAD]).wait()

    def remote(source, target, send_sem, recv_sem, device):
        return pltpu.make_async_remote_copy(
            src_ref=source,
            dst_ref=target,
            send_sem=send_sem,
            recv_sem=recv_sem,
            device_id={"batch": device},
            device_id_type=pl.DeviceIdType.MESH,
        )

    def hop(piece, step):
        i, m, row, rows, x_first = piece
        first = other_x if x_first else other_y
        at = pl.ds(row, rows)
        place = gathered[m]
        half = place.at[:, x, c, at, :] if x_first else place.at[y, :, c, at, :]
        source, target, device = (
            (send_1[i], recv_1[i], other_c),
            (send_2[i], recv_2[i], first),
            (half, half, first),
            (place.at[:, :, c, at, :], place.at[:, :, c, at, :], other_c),
        )[step]
        kind = (CORE, FIRST, LOAD, CORE)[step]
        return remote(source, target, send_sems.at[m], sems.at[i, kind], device)

    def group_hop(group, step):
        g, m, row, rows, x_first, _ = group
        second = other_y if x_first else other_x
        place = gathered[m].at[y, x, c, pl.ds(row, rows), :]
        source, target = ((send_3[g], recv_3[g]), (place, place))[step]
        return remote(source, target, send_sems.at[m], group_sems.at[g, step], second)

    def sent(m):
        width = shapes[m][1]
        part = pl.ds(0, 7) if BY_ROWS[m] else (slice(None), pl.ds(0, 7 * width))
        pltpu.make_async_copy(grads[m].at[part], grad_v[m].at[part], send_sems.at[m]).wait()

    def block(piece, owner):
        _, m, row, rows, _ = piece
        at = pl.ds(row, rows)
        if BY_ROWS[m]:
            return grad_v[m][owner, at, :]
        width = shapes[m][1]
        return grad_v[m][at, pl.ds(pl.multiple_of(owner * width, width), width)]

    def spot(x_first, first, second):
        return 2 * second + first if x_first else 2 * first + second

    def give(piece):
        i = piece[0]
        load(piece).wait()
        for q in range(4):
            send_1[i][q] = block(piece, 2 * q + 1 - c).astype(jnp.bfloat16)

    def add_core(piece):
        i, x_first = piece[0], piece[-1]
        f = x if x_first else y
        hop(piece, 0).wait_recv()
        for second in range(2):
            q = spot(x_first, 1 - f, second)
            total = block(piece, 2 * q + c) + recv_1[i][q].astype(jnp.float32)
            send_2[i][second] = total.astype(jnp.bfloat16)
        hop(piece, 1).start()
        for second in range(2):
            q = spot(x_first, f, second)
            keep_2[i][second] = block(piece, 2 * q + c) + recv_1[i][q].astype(jnp.float32)

    def add_first(group):
        g, m, start, _, x_first, pieces = group
        s = y if x_first else x
        for i, _, row, rows, _ in pieces:
            hop((i, m, row, rows, x_first), 1).wait_recv()
            total = keep_2[i][1 - s] + recv_2[i][1 - s].astype(jnp.float32)
            send_3[g][pl.ds(row - start, rows), :] = total.astype(jnp.bfloat16)
        group_hop(group, 0).start()
        for i, _, row, rows, _ in pieces:
            total = keep_2[i][s] + recv_2[i][s].astype(jnp.float32)
            keep_3[g][pl.ds(row - start, rows), :] = total

    def update(group):
        g, m, row, rows, _, _ = group
        at = pl.ds(row, rows)
        group_hop(group, 0).wait_recv()
        mean = (keep_3[g][...] + recv_3[g][...].astype(jnp.float32)) * rate
        state = hold_rate * param_v[m][1, at, :] + mean
        new = param_v[m][0, at, :] - learn_rate * state
        gathered[m][y, x, c, at, :] = new.astype(jnp.bfloat16)
        group_hop(group, 1).start()
        news[m][at, :] = new
        states[m][at, :] = state

    def spread(group):
        group_hop(group, 1).wait_recv()
        for piece in group[-1]:
            hop(piece, 2).start()

    def pass_on(piece):
        hop(piece, 2).wait_recv()
        hop(piece, 3).start()

    def finish(piece):
        hop(piece, 3).wait_recv()

    def norm_loads():
        return [
            pltpu.make_async_copy(source, target, sems.at[early[6 + i], LOAD])
            for i, (source, target) in enumerate(zip(norm_inputs, norm_held))
        ]

    def norm_hop(step):
        device = (other_c, other_x, other_y)[step]
        return remote(
            norm_send.at[step], norm_recv.at[step], norm_sems.at[3], norm_sems.at[step], device
        )

    def norm_stage(step):
        width = norm_held[1].shape[1]
        if step == 0:
            for copy in norm_loads():
                copy.wait()
            for j in range(n):
                norm_send[0, 0, pl.ds(j, 1), :] = norm_held[0][:, j * width : (j + 1) * width]
            own = lax.broadcasted_iota(jnp.int32, (n, width), 0) == me
            for j in (1, 2):
                norm_send[0, j] = jnp.where(own, jnp.broadcast_to(norm_held[j][...], (n, width)), 0.0)
            norm_hop(0).start()
            return
        norm_hop(step - 1).wait_recv()
        total = norm_send[step - 1] + norm_recv[step - 1]
        if step < 3:
            norm_send[step] = total
            norm_hop(step).start()
            return
        state = hold_rate * total[2] + total[0] * rate
        new = total[1] - learn_rate * state
        norm_copy[...] = new.astype(jnp.bfloat16)
        norm_full[0] = new
        norm_full[1] = state
        norm_new[...] = norm_full[0, pl.ds(me, 1), :]
        norm_state[...] = norm_full[1, pl.ds(me, 1), :]
        remote(norm_send, norm_recv, norm_sems.at[3], norm_sems.at[3], other_c).wait_send()

    def both(act, parts):
        for part in parts:
            act(part)

    in_pairs = list(zip(*streams))
    group_pairs = list(zip(*lists))
    for pair in in_pairs[: LEAD + 1]:
        both(lambda piece: load(piece).start(), pair)
    both(give, in_pairs[0])
    pl.semaphore_wait(barrier, 3)
    both(lambda piece: hop(piece, 0).start(), in_pairs[0])
    for p in range(1, pairs + 1):
        if p < pairs:
            for piece in in_pairs[p]:
                give(piece)
                hop(piece, 0).start()
        if p + LEAD < pairs:
            both(lambda piece: load(piece).start(), in_pairs[p + LEAD])
        if p == pairs - LEAD:
            for m in range(6):
                for copy in params(m):
                    copy.start()
        if p == pairs - 1:
            for copy in norm_loads():
                copy.start()
        both(add_core, in_pairs[p - 1])
    both(params_wait, range(6))
    norm_stage(0)
    for i, pair in enumerate(group_pairs):
        both(add_first, pair)
        if i == 0:
            norm_stage(1)
    norm_stage(2)
    for pair in group_pairs:
        both(update, pair)
    norm_stage(3)
    for pair in group_pairs:
        both(spread, pair)
    for act in (pass_on, finish):
        for pair in in_pairs:
            both(act, pair)
    both(sent, range(6))


def write_out(shapes, n, *refs):
    refs = list(refs)

    def take(count):
        out, refs[:] = refs[:count], refs[count:]
        return out

    gathered, news, states, norms = take(6), take(6), take(6), take(3)
    copies, new_outs, state_outs, norm_outs = take(6), take(6), take(6), take(3)
    sems, norm_sems = take(2)
    for m in range(6):
        if BY_ROWS[m]:
            pltpu.make_async_copy(gathered[m], copies[m], sems.at[m, 0]).start()
        else:
            width = shapes[m][1]
            for j in range(n):
                source = gathered[m].at[j // 4, j // 2 % 2, j % 2]
                target = copies[m].at[:, pl.ds(j * width, width)]
                pltpu.make_async_copy(source, target, sems.at[m, 0]).start()
        pltpu.make_async_copy(news[m], new_outs[m], sems.at[m, 1]).start()
        pltpu.make_async_copy(states[m], state_outs[m], sems.at[m, 1]).start()
    moves = [
        pltpu.make_async_copy(a, b, norm_sems.at[i])
        for i, (a, b) in enumerate(zip(norms, norm_outs))
    ]
    for move in moves:
        move.start()
    for m in range(6):
        every, half = gathered[m], gathered[m].at[0]
        pltpu.make_async_copy(every, every, sems.at[m, 0]).wait()
        pltpu.make_async_copy(half, half, sems.at[m, 1]).wait()
    for move in moves:
        move.wait()


def kernel_body(*args):
    n = lax.axis_size("batch")
    grads, grad_norm = [a[0] for a in args[:6]], args[6]
    weights, weight_norm = args[7:13], args[13]
    moments, moment_norm = args[14:20], args[20]
    shapes = [w.shape for w in weights]
    grads = [g.reshape((n, *s)) if by_rows else g for g, s, by_rows in zip(grads, shapes, BY_ROWS)]
    width = weight_norm.shape[0]
    bf16, f32 = jnp.bfloat16, jnp.float32
    any_spec = pl.BlockSpec(memory_space=pl.ANY)
    vmem_spec = pl.BlockSpec(memory_space=pltpu.VMEM)
    hbm_spec = pl.BlockSpec(memory_space=pltpu.HBM)
    lists = pieces_of(shapes)
    groups = [group for pair in zip(*lists) for group in pair]
    pieces = [piece for groups_s in lists for group in groups_s for piece in group[-1]]
    assert len(groups) == 2 * len(lists[0]) and len(groups) == 2 * len(lists[1])

    def scratch(parts, lead, kind):
        return [pltpu.VMEM((*lead, part[3], shapes[part[1]][1]), kind) for part in parts]

    plain = [jax.ShapeDtypeStruct(s, f32) for s in shapes] * 2 + [
        jax.ShapeDtypeStruct((n, width), bf16),
        jax.ShapeDtypeStruct((1, width), f32),
        jax.ShapeDtypeStruct((1, width), f32),
    ]
    parts = [jax.ShapeDtypeStruct((2, 2, 2, *s), bf16) for s in shapes]
    norms = (grad_norm, weight_norm.reshape(1, width), moment_norm.reshape(1, width))
    arrays = (*grads, *weights, *moments, *norms)
    results = pl.pallas_call(
        functools.partial(exchange, shapes, n),
        out_shape=parts + plain,
        in_specs=[any_spec] * 21,
        out_specs=[vmem_spec] * 21,
        scratch_shapes=[pltpu.VMEM(g.shape, f32) for g in grads]
        + [pltpu.VMEM((2, *s), f32) for s in shapes]
        + scratch(pieces, (4,), bf16) * 2
        + scratch(pieces, (2,), bf16) * 2
        + scratch(pieces, (2,), f32)
        + scratch(groups, (), bf16) * 2
        + scratch(groups, (), f32)
        + [pltpu.VMEM((1, n * width), f32)]
        + [pltpu.VMEM((1, width), f32)] * 2
        + [pltpu.VMEM((3, 3, n, width), f32)] * 2
        + [pltpu.VMEM((2, n, width), f32)]
        + [
            pltpu.SemaphoreType.DMA((len(pieces), KINDS)),
            pltpu.SemaphoreType.DMA((6,)),
            pltpu.SemaphoreType.DMA((len(groups), 2)),
            pltpu.SemaphoreType.DMA((4,)),
        ],
        compiler_params=pltpu.CompilerParams(
            collective_id=0, has_side_effects=True, vmem_limit_bytes=40 * 2**20
        ),
    )(*[pltpu.with_memory_space_constraint(a, pltpu.HBM) for a in arrays])
    finals = pl.pallas_call(
        functools.partial(write_out, shapes, n),
        out_shape=[
            part if by_rows else jax.ShapeDtypeStruct((s[0], n * s[1]), bf16)
            for part, s, by_rows in zip(parts, shapes, BY_ROWS)
        ]
        + plain,
        in_specs=[any_spec] * 21,
        out_specs=[hbm_spec] * 21,
        scratch_shapes=[pltpu.SemaphoreType.DMA((6, 2)), pltpu.SemaphoreType.DMA((3,))],
        compiler_params=pltpu.CompilerParams(vmem_limit_bytes=8 * 2**20),
    )(*[pltpu.with_memory_space_constraint(r, pltpu.VMEM) for r in results])
    copy = [f.reshape(-1, f.shape[-1]) for f in finals[:6]]
    new, state = finals[6:12], finals[12:18]
    copy_norm, new_norm, state_norm = (r.reshape(-1) for r in finals[18:])
    return (*copy, copy_norm, *new, new_norm, *state, state_norm)


def chosen(*args):
    fits = lax.axis_size("batch") == 2**3 and args[13].shape[0] % 128 == 0
    for m, shares in PLANS[0] + PLANS[1]:
        w = args[7 + m]
        fits = fits and w.shape[0] % (16 * sum(map(sum, shares))) == 0 and w.shape[1] % 128 == 0
    return kernel_body(*args) if fits else body(*args)


def solution(mesh):
    in_specs = (
        P("batch", None, "cols"),
        P("batch", "cols", None),
        P("batch", None, "cols"),
        P("batch", None, "cols"),
        P("batch", None, "cols"),
        P("batch", "cols", None),
        P("batch", None),
        P("batch", "cols"),
        P("cols", "batch"),
        P("batch", "cols"),
        P("batch", "cols"),
        P("batch", "cols"),
        P("cols", "batch"),
        P("batch"),
        P("batch", "cols"),
        P("cols", "batch"),
        P("batch", "cols"),
        P("batch", "cols"),
        P("batch", "cols"),
        P("cols", "batch"),
        P("batch"),
    )
    out_specs = (
        P(None, "cols"),
        P("cols", None),
        P(None, "cols"),
        P(None, "cols"),
        P(None, "cols"),
        P("cols", None),
        P(),
        P("batch", "cols"),
        P("cols", "batch"),
        P("batch", "cols"),
        P("batch", "cols"),
        P("batch", "cols"),
        P("cols", "batch"),
        P("batch"),
        P("batch", "cols"),
        P("cols", "batch"),
        P("batch", "cols"),
        P("batch", "cols"),
        P("batch", "cols"),
        P("cols", "batch"),
        P("batch"),
    )
    return jax.shard_map(chosen, mesh=mesh, in_specs=in_specs, out_specs=out_specs, check_vma=False)
```

```python
import functools

import jax
import jax.numpy as jnp
from jax import lax
from jax.experimental import pallas as pl
from jax.experimental.pallas import tpu as pltpu
from jax.sharding import PartitionSpec as P

learn_rate = 0.1
hold_rate = 0.7


def body(
    grad_up,
    grad_down,
    grad_query,
    grad_key,
    grad_value,
    grad_mixed,
    grad_norm,
    weight_up,
    weight_down,
    weight_query,
    weight_key,
    weight_value,
    weight_mixed,
    weight_norm,
    moment_up,
    moment_down,
    moment_query,
    moment_key,
    moment_value,
    moment_mixed,
    moment_norm,
):
    mean_up, mean_down, mean_query, mean_key, mean_value, mean_mixed = (
        lax.psum_scatter(
            grad_up[0].astype(jnp.bfloat16), "batch", scatter_dimension=0, tiled=True
        ).astype(jnp.float32),
        lax.psum_scatter(
            grad_down[0].astype(jnp.bfloat16), "batch", scatter_dimension=1, tiled=True
        ).astype(jnp.float32),
        lax.psum_scatter(
            grad_query[0].astype(jnp.bfloat16), "batch", scatter_dimension=0, tiled=True
        ).astype(jnp.float32),
        lax.psum_scatter(
            grad_key[0].astype(jnp.bfloat16), "batch", scatter_dimension=0, tiled=True
        ).astype(jnp.float32),
        lax.psum_scatter(
            grad_value[0].astype(jnp.bfloat16), "batch", scatter_dimension=0, tiled=True
        ).astype(jnp.float32),
        lax.psum_scatter(
            grad_mixed[0].astype(jnp.bfloat16), "batch", scatter_dimension=1, tiled=True
        ).astype(jnp.float32),
    )
    whole_norm = lax.psum(grad_norm[0], "batch")
    place = lax.axis_index("batch")
    mean_norm = lax.dynamic_slice_in_dim(
        whole_norm, place * weight_norm.shape[0], weight_norm.shape[0]
    )
    mean_rate = lax.axis_size("batch") ** (-0.5)
    mean_up = mean_up * mean_rate
    mean_down = mean_down * mean_rate
    mean_query = mean_query * mean_rate
    mean_key = mean_key * mean_rate
    mean_value = mean_value * mean_rate
    mean_mixed = mean_mixed * mean_rate
    mean_norm = mean_norm * mean_rate
    state_new_up = hold_rate * moment_up + mean_up
    new_up = weight_up - learn_rate * state_new_up
    state_new_down = hold_rate * moment_down + mean_down
    new_down = weight_down - learn_rate * state_new_down
    state_new_query = hold_rate * moment_query + mean_query
    new_query = weight_query - learn_rate * state_new_query
    state_new_key = hold_rate * moment_key + mean_key
    new_key = weight_key - learn_rate * state_new_key
    state_new_value = hold_rate * moment_value + mean_value
    new_value = weight_value - learn_rate * state_new_value
    state_new_mixed = hold_rate * moment_mixed + mean_mixed
    new_mixed = weight_mixed - learn_rate * state_new_mixed
    state_new_norm = hold_rate * moment_norm + mean_norm
    new_norm = weight_norm - learn_rate * state_new_norm
    copy_up, copy_down, copy_query, copy_key, copy_value, copy_mixed, copy_norm = (
        lax.all_gather(new_up.astype(jnp.bfloat16), "batch", axis=0, tiled=True),
        lax.all_gather(new_down.astype(jnp.bfloat16), "batch", axis=1, tiled=True),
        lax.all_gather(new_query.astype(jnp.bfloat16), "batch", axis=0, tiled=True),
        lax.all_gather(new_key.astype(jnp.bfloat16), "batch", axis=0, tiled=True),
        lax.all_gather(new_value.astype(jnp.bfloat16), "batch", axis=0, tiled=True),
        lax.all_gather(new_mixed.astype(jnp.bfloat16), "batch", axis=1, tiled=True),
        lax.all_gather(new_norm.astype(jnp.bfloat16), "batch", axis=0, tiled=True),
    )
    return (
        copy_up,
        copy_down,
        copy_query,
        copy_key,
        copy_value,
        copy_mixed,
        copy_norm,
        new_up,
        new_down,
        new_query,
        new_key,
        new_value,
        new_mixed,
        new_norm,
        state_new_up,
        state_new_down,
        state_new_query,
        state_new_key,
        state_new_value,
        state_new_mixed,
        state_new_norm,
    )


PLANS = (((2, ((1, 3),)), (0, ((1, 1), (2,))), (3, ((3, 1),))), ((4, ((1, 3),)), (1, ((1, 1), (2,))), (5, ((3, 1),))))
LEAD = 2
LATE = 4
BY_ROWS = (True, False, True, True, True, False)
LOAD, CORE, FIRST, KINDS = 0, 1, 2, 3


def pieces_of(shapes):
    lists = []
    count = 0
    for s, plan in enumerate(PLANS):
        lists.append([])
        for m, shares in plan:
            row = 0
            unit = shapes[m][0] // sum(map(sum, shares))
            for group in shares:
                start, pieces = row, []
                for share in group:
                    pieces.append((count, m, row, unit * share, s == 0))
                    row += unit * share
                    count += 1
                lists[s].append((2 * len(lists[s]) + s, m, start, row - start, s == 0, pieces))
    return lists


def exchange(shapes, n, *refs):
    refs = list(refs)

    def take(count):
        out, refs[:] = refs[:count], refs[count:]
        return out

    lists = pieces_of(shapes)
    groups = len(lists[0])
    streams = [[piece for group in groups_s for piece in group[-1]] for groups_s in lists]
    pairs = len(streams[0])
    head = [stream[0] for stream in streams]
    last = [stream[-1] for stream in streams]
    early = [piece[0] for pair in zip(*streams) for piece in pair]
    grads, weights, moments = take(6), take(6), take(6)
    norm_inputs = take(3)
    gathered, news, states = take(6), take(6), take(6)
    norm_copy, norm_new, norm_state = take(3)
    grad_v, param_v = take(6), take(6)
    send_1, recv_1, send_2, recv_2, keep_2 = (take(2 * pairs) for _ in range(5))
    send_3, recv_3, keep_3 = (take(2 * groups) for _ in range(3))
    norm_held = take(3)
    norm_send, norm_recv, norm_full = take(3)
    sems, send_sems, group_sems, norm_sems, cross_sems = take(5)

    me = lax.axis_index("batch")
    c = lax.rem(me, 2)
    x = lax.rem(lax.div(me, 2), 2)
    y = lax.div(me, 4)
    other_c, other_x, other_y = me + 1 - 2 * c, me + 2 - 4 * x, me + 4 - 8 * y
    rate = n ** (-0.5)

    barrier = pltpu.get_barrier_semaphore()
    for device in (other_c, other_x, other_y):
        pl.semaphore_signal(
            barrier, inc=1, device_id={"batch": device}, device_id_type=pl.DeviceIdType.MESH
        )

    def load(piece):
        i, m, row, rows, _ = piece
        at = pl.ds(row, rows)
        if BY_ROWS[m]:
            source, target = grads[m].at[:, at, :], grad_v[m].at[:, at, :]
        else:
            source, target = grads[m].at[at, :], grad_v[m].at[at, :]
        return pltpu.make_async_copy(source, target, sems.at[i, LOAD])

    def params(m):
        sem = sems.at[early[m], LOAD]
        return (
            pltpu.make_async_copy(weights[m], param_v[m].at[0], sem),
            pltpu.make_async_copy(moments[m], param_v[m].at[1], sem),
        )

    def params_wait(m):
        pltpu.make_async_copy(param_v[m], param_v[m], sems.at[early[m], LOAD]).wait()

    def remote(source, target, send_sem, recv_sem, device):
        return pltpu.make_async_remote_copy(
            src_ref=source,
            dst_ref=target,
            send_sem=send_sem,
            recv_sem=recv_sem,
            device_id={"batch": device},
            device_id_type=pl.DeviceIdType.MESH,
        )

    def hop(piece, step):
        i, m, row, rows, x_first = piece
        first = other_x if x_first else other_y
        at = pl.ds(row, rows)
        place = gathered[m]
        full = place.at[:, :, c, at, :]
        half = place.at[:, x, c, at, :] if x_first else place.at[y, :, c, at, :]
        source, target, device = (
            (send_1[i], recv_1[i], first if piece in head else other_c),
            (send_2[i], recv_2[i], other_c if piece in head else first),
            (half, half, first),
            (half, half, other_c) if piece in last else (full, full, other_c),
        )[step]
        kind = (CORE, FIRST, LOAD, CORE)[step]
        return remote(source, target, send_sems.at[m], sems.at[i, kind], device)

    def cross_hop(piece):
        i, m, row, rows, x_first = piece
        at = pl.ds(row, rows)
        half = gathered[m].at[:, x, c, at, :] if x_first else gathered[m].at[y, :, c, at, :]
        device = (other_x if x_first else other_y) + 1 - 2 * c
        return remote(half, half, send_sems.at[m], cross_sems.at[0 if x_first else 1], device)

    def group_hop(group, step):
        g, m, row, rows, x_first, _ = group
        second = other_y if x_first else other_x
        place = gathered[m].at[y, x, c, pl.ds(row, rows), :]
        source, target = ((send_3[g], recv_3[g]), (place, place))[step]
        return remote(source, target, send_sems.at[m], group_sems.at[g, step], second)

    def sent(m):
        width = shapes[m][1]
        part = pl.ds(0, 7) if BY_ROWS[m] else (slice(None), pl.ds(0, 7 * width))
        pltpu.make_async_copy(grads[m].at[part], grad_v[m].at[part], send_sems.at[m]).wait()

    def block(piece, owner):
        _, m, row, rows, _ = piece
        at = pl.ds(row, rows)
        if BY_ROWS[m]:
            return grad_v[m][owner, at, :]
        width = shapes[m][1]
        return grad_v[m][at, pl.ds(pl.multiple_of(owner * width, width), width)]

    def spot(x_first, first, second):
        return 2 * second + first if x_first else 2 * first + second

    def shares(piece):
        f = x if piece[-1] else y

        def owner(first, second, core):
            return 2 * spot(piece[-1], first, second) + core

        if piece in head:
            return (
                [owner(1 - f, q // 2, q % 2) for q in range(4)],
                [(owner(f, second, 1 - c), 2 * second + 1 - c) for second in range(2)],
                [(owner(f, second, c), 2 * second + c) for second in range(2)],
            )
        return (
            [2 * q + 1 - c for q in range(4)],
            [(owner(1 - f, second, c), spot(piece[-1], 1 - f, second)) for second in range(2)],
            [(owner(f, second, c), spot(piece[-1], f, second)) for second in range(2)],
        )

    def give(piece):
        load(piece).wait()
        for q, owner in enumerate(shares(piece)[0]):
            send_1[piece[0]][q] = block(piece, owner).astype(jnp.bfloat16)

    def add_core(piece):
        i = piece[0]
        _, given, kept = shares(piece)
        hop(piece, 0).wait_recv()
        for j, (owner, q) in enumerate(given):
            total = block(piece, owner) + recv_1[i][q].astype(jnp.float32)
            send_2[i][j] = total.astype(jnp.bfloat16)
        hop(piece, 1).start()
        for j, (owner, q) in enumerate(kept):
            keep_2[i][j] = block(piece, owner) + recv_1[i][q].astype(jnp.float32)

    def add_first(group):
        g, m, start, _, x_first, pieces = group
        s = y if x_first else x
        for i, _, row, rows, _ in pieces:
            hop((i, m, row, rows, x_first), 1).wait_recv()
            total = keep_2[i][1 - s] + recv_2[i][1 - s].astype(jnp.float32)
            send_3[g][pl.ds(row - start, rows), :] = total.astype(jnp.bfloat16)
        group_hop(group, 0).start()
        for i, _, row, rows, _ in pieces:
            total = keep_2[i][s] + recv_2[i][s].astype(jnp.float32)
            keep_3[g][pl.ds(row - start, rows), :] = total

    def update(group):
        g, m, row, rows, _, _ = group
        at = pl.ds(row, rows)
        group_hop(group, 0).wait_recv()
        mean = (keep_3[g][...] + recv_3[g][...].astype(jnp.float32)) * rate
        state = hold_rate * param_v[m][1, at, :] + mean
        new = param_v[m][0, at, :] - learn_rate * state
        gathered[m][y, x, c, at, :] = new.astype(jnp.bfloat16)
        group_hop(group, 1).start()
        news[m][at, :] = new
        states[m][at, :] = state

    def spread(group):
        group_hop(group, 1).wait_recv()
        for piece in group[-1]:
            hop(piece, 2).start()
            if piece in last:
                cross_hop(piece).start()
                hop(piece, 3).start()

    def pass_on(piece):
        if piece not in last:
            hop(piece, 2).wait_recv()
            hop(piece, 3).start()

    def finish(piece):
        if piece in last:
            hop(piece, 2).wait_recv()
            cross_hop(piece).wait_recv()
        hop(piece, 3).wait_recv()

    def norm_loads():
        return [
            pltpu.make_async_copy(source, target, sems.at[early[6 + i], LOAD])
            for i, (source, target) in enumerate(zip(norm_inputs, norm_held))
        ]

    def norm_hop(step):
        device = (other_c, other_x, other_y)[step]
        return remote(
            norm_send.at[step], norm_recv.at[step], norm_sems.at[3], norm_sems.at[step], device
        )

    def norm_stage(step):
        width = norm_held[1].shape[1]
        if step == 0:
            for copy in norm_loads():
                copy.wait()
            for j in range(n):
                norm_send[0, 0, pl.ds(j, 1), :] = norm_held[0][:, j * width : (j + 1) * width]
            own = lax.broadcasted_iota(jnp.int32, (n, width), 0) == me
            for j in (1, 2):
                norm_send[0, j] = jnp.where(own, jnp.broadcast_to(norm_held[j][...], (n, width)), 0.0)
            norm_hop(0).start()
            return
        norm_hop(step - 1).wait_recv()
        total = norm_send[step - 1] + norm_recv[step - 1]
        if step < 3:
            norm_send[step] = total
            norm_hop(step).start()
            return
        state = hold_rate * total[2] + total[0] * rate
        new = total[1] - learn_rate * state
        norm_copy[...] = new.astype(jnp.bfloat16)
        norm_full[0] = new
        norm_full[1] = state
        norm_new[...] = norm_full[0, pl.ds(me, 1), :]
        norm_state[...] = norm_full[1, pl.ds(me, 1), :]
        remote(norm_send, norm_recv, norm_sems.at[3], norm_sems.at[3], other_c).wait_send()

    def both(act, parts):
        for part in parts:
            act(part)

    in_pairs = list(zip(*streams))
    group_pairs = list(zip(*lists))
    for pair in in_pairs[: LEAD + 1]:
        both(lambda piece: load(piece).start(), pair)
    both(give, in_pairs[0])
    pl.semaphore_wait(barrier, 3)
    both(lambda piece: hop(piece, 0).start(), in_pairs[0])
    for p in range(1, pairs + 1):
        if p < pairs:
            for piece in in_pairs[p]:
                give(piece)
                hop(piece, 0).start()
        if p + LEAD < pairs:
            both(lambda piece: load(piece).start(), in_pairs[p + LEAD])
        if p == pairs - LEAD:
            for m in range(6):
                for copy in params(m):
                    copy.start()
        if p == pairs - 1:
            for copy in norm_loads():
                copy.start()
        if p > 1:
            both(add_core, in_pairs[p - 1])
        if p == LATE:
            both(add_core, in_pairs[0])
    both(params_wait, range(6))
    norm_stage(0)
    for i, pair in enumerate(group_pairs):
        both(add_first, pair)
        if i == 0:
            norm_stage(1)
    norm_stage(2)
    for pair in group_pairs:
        both(update, pair)
    norm_stage(3)
    for pair in group_pairs:
        both(spread, pair)
    for act in (pass_on, finish):
        for pair in in_pairs:
            both(act, pair)
    both(sent, range(6))


def write_out(shapes, n, *refs):
    refs = list(refs)

    def take(count):
        out, refs[:] = refs[:count], refs[count:]
        return out

    gathered, news, states, norms = take(6), take(6), take(6), take(3)
    copies, new_outs, state_outs, norm_outs = take(6), take(6), take(6), take(3)
    sems, norm_sems = take(2)
    for m in range(6):
        if BY_ROWS[m]:
            pltpu.make_async_copy(gathered[m], copies[m], sems.at[m, 0]).start()
        else:
            width = shapes[m][1]
            for j in range(n):
                source = gathered[m].at[j // 4, j // 2 % 2, j % 2]
                target = copies[m].at[:, pl.ds(j * width, width)]
                pltpu.make_async_copy(source, target, sems.at[m, 0]).start()
        pltpu.make_async_copy(news[m], new_outs[m], sems.at[m, 1]).start()
        pltpu.make_async_copy(states[m], state_outs[m], sems.at[m, 1]).start()
    moves = [
        pltpu.make_async_copy(a, b, norm_sems.at[i])
        for i, (a, b) in enumerate(zip(norms, norm_outs))
    ]
    for move in moves:
        move.start()
    for m in range(6):
        every, half = gathered[m], gathered[m].at[0]
        pltpu.make_async_copy(every, every, sems.at[m, 0]).wait()
        pltpu.make_async_copy(half, half, sems.at[m, 1]).wait()
    for move in moves:
        move.wait()


def kernel_body(*args):
    n = lax.axis_size("batch")
    grads, grad_norm = [a[0] for a in args[:6]], args[6]
    weights, weight_norm = args[7:13], args[13]
    moments, moment_norm = args[14:20], args[20]
    shapes = [w.shape for w in weights]
    grads = [g.reshape((n, *s)) if by_rows else g for g, s, by_rows in zip(grads, shapes, BY_ROWS)]
    width = weight_norm.shape[0]
    bf16, f32 = jnp.bfloat16, jnp.float32
    any_spec = pl.BlockSpec(memory_space=pl.ANY)
    vmem_spec = pl.BlockSpec(memory_space=pltpu.VMEM)
    hbm_spec = pl.BlockSpec(memory_space=pltpu.HBM)
    lists = pieces_of(shapes)
    groups = [group for pair in zip(*lists) for group in pair]
    pieces = [piece for groups_s in lists for group in groups_s for piece in group[-1]]
    assert len(groups) == 2 * len(lists[0]) and len(groups) == 2 * len(lists[1])

    def scratch(parts, lead, kind):
        return [pltpu.VMEM((*lead, part[3], shapes[part[1]][1]), kind) for part in parts]

    plain = [jax.ShapeDtypeStruct(s, f32) for s in shapes] * 2 + [
        jax.ShapeDtypeStruct((n, width), bf16),
        jax.ShapeDtypeStruct((1, width), f32),
        jax.ShapeDtypeStruct((1, width), f32),
    ]
    parts = [jax.ShapeDtypeStruct((2, 2, 2, *s), bf16) for s in shapes]
    norms = (grad_norm, weight_norm.reshape(1, width), moment_norm.reshape(1, width))
    arrays = (*grads, *weights, *moments, *norms)
    results = pl.pallas_call(
        functools.partial(exchange, shapes, n),
        out_shape=parts + plain,
        in_specs=[any_spec] * 21,
        out_specs=[vmem_spec] * 21,
        scratch_shapes=[pltpu.VMEM(g.shape, f32) for g in grads]
        + [pltpu.VMEM((2, *s), f32) for s in shapes]
        + scratch(pieces, (4,), bf16) * 2
        + scratch(pieces, (2,), bf16) * 2
        + scratch(pieces, (2,), f32)
        + scratch(groups, (), bf16) * 2
        + scratch(groups, (), f32)
        + [pltpu.VMEM((1, n * width), f32)]
        + [pltpu.VMEM((1, width), f32)] * 2
        + [pltpu.VMEM((3, 3, n, width), f32)] * 2
        + [pltpu.VMEM((2, n, width), f32)]
        + [
            pltpu.SemaphoreType.DMA((len(pieces), KINDS)),
            pltpu.SemaphoreType.DMA((6,)),
            pltpu.SemaphoreType.DMA((len(groups), 2)),
            pltpu.SemaphoreType.DMA((4,)),
            pltpu.SemaphoreType.DMA((2,)),
        ],
        compiler_params=pltpu.CompilerParams(
            collective_id=0, has_side_effects=True, vmem_limit_bytes=40 * 2**20
        ),
    )(*[pltpu.with_memory_space_constraint(a, pltpu.HBM) for a in arrays])
    finals = pl.pallas_call(
        functools.partial(write_out, shapes, n),
        out_shape=[
            part if by_rows else jax.ShapeDtypeStruct((s[0], n * s[1]), bf16)
            for part, s, by_rows in zip(parts, shapes, BY_ROWS)
        ]
        + plain,
        in_specs=[any_spec] * 21,
        out_specs=[hbm_spec] * 21,
        scratch_shapes=[pltpu.SemaphoreType.DMA((6, 2)), pltpu.SemaphoreType.DMA((3,))],
        compiler_params=pltpu.CompilerParams(vmem_limit_bytes=8 * 2**20),
    )(*[pltpu.with_memory_space_constraint(r, pltpu.VMEM) for r in results])
    copy = [f.reshape(-1, f.shape[-1]) for f in finals[:6]]
    new, state = finals[6:12], finals[12:18]
    copy_norm, new_norm, state_norm = (r.reshape(-1) for r in finals[18:])
    return (*copy, copy_norm, *new, new_norm, *state, state_norm)


def chosen(*args):
    fits = lax.axis_size("batch") == 2**3 and args[13].shape[0] % 128 == 0
    for m, shares in PLANS[0] + PLANS[1]:
        w = args[7 + m]
        fits = fits and w.shape[0] % (16 * sum(map(sum, shares))) == 0 and w.shape[1] % 128 == 0
    return kernel_body(*args) if fits else body(*args)


def solution(mesh):
    in_specs = (
        P("batch", None, "cols"),
        P("batch", "cols", None),
        P("batch", None, "cols"),
        P("batch", None, "cols"),
        P("batch", None, "cols"),
        P("batch", "cols", None),
        P("batch", None),
        P("batch", "cols"),
        P("cols", "batch"),
        P("batch", "cols"),
        P("batch", "cols"),
        P("batch", "cols"),
        P("cols", "batch"),
        P("batch"),
        P("batch", "cols"),
        P("cols", "batch"),
        P("batch", "cols"),
        P("batch", "cols"),
        P("batch", "cols"),
        P("cols", "batch"),
        P("batch"),
    )
    out_specs = (
        P(None, "cols"),
        P("cols", None),
        P(None, "cols"),
        P(None, "cols"),
        P(None, "cols"),
        P("cols", None),
        P(),
        P("batch", "cols"),
        P("cols", "batch"),
        P("batch", "cols"),
        P("batch", "cols"),
        P("batch", "cols"),
        P("cols", "batch"),
        P("batch"),
        P("batch", "cols"),
        P("cols", "batch"),
        P("batch", "cols"),
        P("batch", "cols"),
        P("batch", "cols"),
        P("cols", "batch"),
        P("batch"),
    )
    return jax.shard_map(chosen, mesh=mesh, in_specs=in_specs, out_specs=out_specs, check_vma=False)
```

```python
import functools

import jax
import jax.numpy as jnp
from jax import lax
from jax.experimental import pallas as pl
from jax.experimental.pallas import tpu as pltpu
from jax.sharding import PartitionSpec as P

learn_rate = 0.1
hold_rate = 0.7


def body(
    grad_up,
    grad_down,
    grad_query,
    grad_key,
    grad_value,
    grad_mixed,
    grad_norm,
    weight_up,
    weight_down,
    weight_query,
    weight_key,
    weight_value,
    weight_mixed,
    weight_norm,
    moment_up,
    moment_down,
    moment_query,
    moment_key,
    moment_value,
    moment_mixed,
    moment_norm,
):
    mean_up, mean_down, mean_query, mean_key, mean_value, mean_mixed = (
        lax.psum_scatter(
            grad_up[0].astype(jnp.bfloat16), "batch", scatter_dimension=0, tiled=True
        ).astype(jnp.float32),
        lax.psum_scatter(
            grad_down[0].astype(jnp.bfloat16), "batch", scatter_dimension=1, tiled=True
        ).astype(jnp.float32),
        lax.psum_scatter(
            grad_query[0].astype(jnp.bfloat16), "batch", scatter_dimension=0, tiled=True
        ).astype(jnp.float32),
        lax.psum_scatter(
            grad_key[0].astype(jnp.bfloat16), "batch", scatter_dimension=0, tiled=True
        ).astype(jnp.float32),
        lax.psum_scatter(
            grad_value[0].astype(jnp.bfloat16), "batch", scatter_dimension=0, tiled=True
        ).astype(jnp.float32),
        lax.psum_scatter(
            grad_mixed[0].astype(jnp.bfloat16), "batch", scatter_dimension=1, tiled=True
        ).astype(jnp.float32),
    )
    whole_norm = lax.psum(grad_norm[0], "batch")
    place = lax.axis_index("batch")
    mean_norm = lax.dynamic_slice_in_dim(
        whole_norm, place * weight_norm.shape[0], weight_norm.shape[0]
    )
    mean_rate = lax.axis_size("batch") ** (-0.5)
    mean_up = mean_up * mean_rate
    mean_down = mean_down * mean_rate
    mean_query = mean_query * mean_rate
    mean_key = mean_key * mean_rate
    mean_value = mean_value * mean_rate
    mean_mixed = mean_mixed * mean_rate
    mean_norm = mean_norm * mean_rate
    state_new_up = hold_rate * moment_up + mean_up
    new_up = weight_up - learn_rate * state_new_up
    state_new_down = hold_rate * moment_down + mean_down
    new_down = weight_down - learn_rate * state_new_down
    state_new_query = hold_rate * moment_query + mean_query
    new_query = weight_query - learn_rate * state_new_query
    state_new_key = hold_rate * moment_key + mean_key
    new_key = weight_key - learn_rate * state_new_key
    state_new_value = hold_rate * moment_value + mean_value
    new_value = weight_value - learn_rate * state_new_value
    state_new_mixed = hold_rate * moment_mixed + mean_mixed
    new_mixed = weight_mixed - learn_rate * state_new_mixed
    state_new_norm = hold_rate * moment_norm + mean_norm
    new_norm = weight_norm - learn_rate * state_new_norm
    copy_up, copy_down, copy_query, copy_key, copy_value, copy_mixed, copy_norm = (
        lax.all_gather(new_up.astype(jnp.bfloat16), "batch", axis=0, tiled=True),
        lax.all_gather(new_down.astype(jnp.bfloat16), "batch", axis=1, tiled=True),
        lax.all_gather(new_query.astype(jnp.bfloat16), "batch", axis=0, tiled=True),
        lax.all_gather(new_key.astype(jnp.bfloat16), "batch", axis=0, tiled=True),
        lax.all_gather(new_value.astype(jnp.bfloat16), "batch", axis=0, tiled=True),
        lax.all_gather(new_mixed.astype(jnp.bfloat16), "batch", axis=1, tiled=True),
        lax.all_gather(new_norm.astype(jnp.bfloat16), "batch", axis=0, tiled=True),
    )
    return (
        copy_up,
        copy_down,
        copy_query,
        copy_key,
        copy_value,
        copy_mixed,
        copy_norm,
        new_up,
        new_down,
        new_query,
        new_key,
        new_value,
        new_mixed,
        new_norm,
        state_new_up,
        state_new_down,
        state_new_query,
        state_new_key,
        state_new_value,
        state_new_mixed,
        state_new_norm,
    )


PLANS = (((2, ((1, 3),)), (0, ((1, 1), (2,))), (3, ((3, 1),))), ((4, ((1, 3),)), (1, ((1, 1), (2,))), (5, ((3, 1),))))
LEAD = 2
LATE = 3
BY_ROWS = (True, False, True, True, True, False)
LOAD, CORE, FIRST, KINDS = 0, 1, 2, 3


def pieces_of(shapes):
    lists = []
    count = 0
    for s, plan in enumerate(PLANS):
        lists.append([])
        for m, shares in plan:
            row = 0
            unit = shapes[m][0] // sum(map(sum, shares))
            for group in shares:
                start, pieces = row, []
                for share in group:
                    pieces.append((count, m, row, unit * share, s == 0))
                    row += unit * share
                    count += 1
                lists[s].append((2 * len(lists[s]) + s, m, start, row - start, s == 0, pieces))
    return lists


def exchange(shapes, n, *refs):
    refs = list(refs)

    def take(count):
        out, refs[:] = refs[:count], refs[count:]
        return out

    lists = pieces_of(shapes)
    groups = len(lists[0])
    streams = [[piece for group in groups_s for piece in group[-1]] for groups_s in lists]
    pairs = len(streams[0])
    head = [stream[0] for stream in streams]
    last = [stream[-1] for stream in streams]
    early = [piece[0] for pair in zip(*streams) for piece in pair]
    grads, weights, moments = take(6), take(6), take(6)
    norm_inputs = take(3)
    gathered, news, states = take(6), take(6), take(6)
    norm_copy, norm_new, norm_state = take(3)
    grad_v, param_v = take(6), take(6)
    send_1, recv_1, send_2, recv_2, keep_2 = (take(2 * pairs) for _ in range(5))
    send_3, recv_3, keep_3 = (take(2 * groups) for _ in range(3))
    norm_held = take(3)
    norm_send, norm_recv, norm_full = take(3)
    sems, send_sems, group_sems, norm_sems, cross_sems = take(5)

    me = lax.axis_index("batch")
    c = lax.rem(me, 2)
    x = lax.rem(lax.div(me, 2), 2)
    y = lax.div(me, 4)
    other_c, other_x, other_y = me + 1 - 2 * c, me + 2 - 4 * x, me + 4 - 8 * y
    rate = n ** (-0.5)

    barrier = pltpu.get_barrier_semaphore()
    for device in (other_c, other_x, other_y):
        pl.semaphore_signal(
            barrier, inc=1, device_id={"batch": device}, device_id_type=pl.DeviceIdType.MESH
        )

    def load(piece):
        i, m, row, rows, _ = piece
        at = pl.ds(row, rows)
        if BY_ROWS[m]:
            source, target = grads[m].at[:, at, :], grad_v[m].at[:, at, :]
        else:
            source, target = grads[m].at[at, :], grad_v[m].at[at, :]
        return pltpu.make_async_copy(source, target, sems.at[i, LOAD])

    def params(m):
        sem = sems.at[early[m], LOAD]
        return (
            pltpu.make_async_copy(weights[m], param_v[m].at[0], sem),
            pltpu.make_async_copy(moments[m], param_v[m].at[1], sem),
        )

    def params_wait(m):
        pltpu.make_async_copy(param_v[m], param_v[m], sems.at[early[m], LOAD]).wait()

    def remote(source, target, send_sem, recv_sem, device):
        return pltpu.make_async_remote_copy(
            src_ref=source,
            dst_ref=target,
            send_sem=send_sem,
            recv_sem=recv_sem,
            device_id={"batch": device},
            device_id_type=pl.DeviceIdType.MESH,
        )

    def hop(piece, step):
        i, m, row, rows, x_first = piece
        first = other_x if x_first else other_y
        at = pl.ds(row, rows)
        place = gathered[m]
        full = place.at[:, :, c, at, :]
        half = place.at[:, x, c, at, :] if x_first else place.at[y, :, c, at, :]
        source, target, device = (
            (send_1[i], recv_1[i], first if piece in head else other_c),
            (send_2[i], recv_2[i], other_c if piece in head else first),
            (half, half, first),
            (half, half, other_c) if piece in last else (full, full, other_c),
        )[step]
        kind = (CORE, FIRST, LOAD, CORE)[step]
        return remote(source, target, send_sems.at[m], sems.at[i, kind], device)

    def cross_hop(piece):
        i, m, row, rows, x_first = piece
        at = pl.ds(row, rows)
        half = gathered[m].at[:, x, c, at, :] if x_first else gathered[m].at[y, :, c, at, :]
        device = (other_x if x_first else other_y) + 1 - 2 * c
        return remote(half, half, send_sems.at[m], cross_sems.at[0 if x_first else 1], device)

    def group_hop(group, step):
        g, m, row, rows, x_first, pieces = group
        second = other_y if x_first else other_x
        place = gathered[m].at[y, x, c, pl.ds(row, rows), :]
        source, target = ((send_3[g], recv_3[g]), (place, place))[step]
        recv_sem = (group_sems.at[g], sems.at[pieces[0][0], FIRST])[step]
        return remote(source, target, send_sems.at[m], recv_sem, second)

    def sent(m):
        width = shapes[m][1]
        part = pl.ds(0, 7) if BY_ROWS[m] else (slice(None), pl.ds(0, 7 * width))
        pltpu.make_async_copy(grads[m].at[part], grad_v[m].at[part], send_sems.at[m]).wait()

    def block(piece, owner):
        _, m, row, rows, _ = piece
        at = pl.ds(row, rows)
        if BY_ROWS[m]:
            return grad_v[m][owner, at, :]
        width = shapes[m][1]
        return grad_v[m][at, pl.ds(pl.multiple_of(owner * width, width), width)]

    def spot(x_first, first, second):
        return 2 * second + first if x_first else 2 * first + second

    def shares(piece):
        f = x if piece[-1] else y

        def owner(first, second, core):
            return 2 * spot(piece[-1], first, second) + core

        if piece in head:
            return (
                [owner(1 - f, q // 2, q % 2) for q in range(4)],
                [(owner(f, second, 1 - c), 2 * second + 1 - c) for second in range(2)],
                [(owner(f, second, c), 2 * second + c) for second in range(2)],
            )
        return (
            [2 * q + 1 - c for q in range(4)],
            [(owner(1 - f, second, c), spot(piece[-1], 1 - f, second)) for second in range(2)],
            [(owner(f, second, c), spot(piece[-1], f, second)) for second in range(2)],
        )

    def give(piece):
        load(piece).wait()
        for q, owner in enumerate(shares(piece)[0]):
            send_1[piece[0]][q] = block(piece, owner).astype(jnp.bfloat16)

    def add_core(piece):
        i = piece[0]
        _, given, kept = shares(piece)
        hop(piece, 0).wait_recv()
        for j, (owner, q) in enumerate(given):
            total = block(piece, owner) + recv_1[i][q].astype(jnp.float32)
            send_2[i][j] = total.astype(jnp.bfloat16)
        hop(piece, 1).start()
        for j, (owner, q) in enumerate(kept):
            keep_2[i][j] = block(piece, owner) + recv_1[i][q].astype(jnp.float32)

    def add_first(group):
        g, m, start, _, x_first, pieces = group
        s = y if x_first else x
        for i, _, row, rows, _ in pieces:
            hop((i, m, row, rows, x_first), 1).wait_recv()
            total = keep_2[i][1 - s] + recv_2[i][1 - s].astype(jnp.float32)
            send_3[g][pl.ds(row - start, rows), :] = total.astype(jnp.bfloat16)
        group_hop(group, 0).start()
        for i, _, row, rows, _ in pieces:
            total = keep_2[i][s] + recv_2[i][s].astype(jnp.float32)
            keep_3[g][pl.ds(row - start, rows), :] = total

    def update(group):
        g, m, row, rows, _, _ = group
        at = pl.ds(row, rows)
        group_hop(group, 0).wait_recv()
        mean = (keep_3[g][...] + recv_3[g][...].astype(jnp.float32)) * rate
        state = hold_rate * param_v[m][1, at, :] + mean
        new = param_v[m][0, at, :] - learn_rate * state
        gathered[m][y, x, c, at, :] = new.astype(jnp.bfloat16)
        group_hop(group, 1).start()
        news[m][at, :] = new
        states[m][at, :] = state

    def spread(group):
        group_hop(group, 1).wait_recv()
        for piece in group[-1]:
            hop(piece, 2).start()
            if piece in last:
                cross_hop(piece).start()
                hop(piece, 3).start()

    def pass_on(piece):
        if piece not in last:
            hop(piece, 2).wait_recv()
            hop(piece, 3).start()

    def finish(piece):
        if piece in last:
            hop(piece, 2).wait_recv()
            cross_hop(piece).wait_recv()
        hop(piece, 3).wait_recv()

    def norm_loads():
        return [
            pltpu.make_async_copy(source, target, sems.at[early[6 + i], LOAD])
            for i, (source, target) in enumerate(zip(norm_inputs, norm_held))
        ]

    def norm_hop(step):
        device = (other_c, other_x, other_y)[step]
        return remote(
            norm_send.at[step], norm_recv.at[step], norm_sems.at[3], norm_sems.at[step], device
        )

    def norm_stage(step):
        width = norm_held[1].shape[1]
        if step == 0:
            for copy in norm_loads():
                copy.wait()
            for j in range(n):
                norm_send[0, 0, pl.ds(j, 1), :] = norm_held[0][:, j * width : (j + 1) * width]
            own = lax.broadcasted_iota(jnp.int32, (n, width), 0) == me
            for j in (1, 2):
                norm_send[0, j] = jnp.where(own, jnp.broadcast_to(norm_held[j][...], (n, width)), 0.0)
            norm_hop(0).start()
            return
        norm_hop(step - 1).wait_recv()
        total = norm_send[step - 1] + norm_recv[step - 1]
        if step < 3:
            norm_send[step] = total
            norm_hop(step).start()
            return
        state = hold_rate * total[2] + total[0] * rate
        new = total[1] - learn_rate * state
        norm_copy[...] = new.astype(jnp.bfloat16)
        norm_full[0] = new
        norm_full[1] = state
        norm_new[...] = norm_full[0, pl.ds(me, 1), :]
        norm_state[...] = norm_full[1, pl.ds(me, 1), :]
        remote(norm_send, norm_recv, norm_sems.at[3], norm_sems.at[3], other_c).wait_send()

    def both(act, parts):
        for part in parts:
            act(part)

    in_pairs = list(zip(*streams))
    group_pairs = list(zip(*lists))
    for pair in in_pairs[: LEAD + 1]:
        both(lambda piece: load(piece).start(), pair)
    both(give, in_pairs[0])
    pl.semaphore_wait(barrier, 3)
    both(lambda piece: hop(piece, 0).start(), in_pairs[0])
    for p in range(1, pairs + 1):
        if p < pairs:
            for piece in in_pairs[p]:
                give(piece)
                hop(piece, 0).start()
        if p + LEAD < pairs:
            both(lambda piece: load(piece).start(), in_pairs[p + LEAD])
        if p == pairs - LEAD:
            for m in range(6):
                for copy in params(m):
                    copy.start()
        if p == pairs - 1:
            for copy in norm_loads():
                copy.start()
        if p > 1:
            both(add_core, in_pairs[p - 1])
        if p == LATE:
            both(add_core, in_pairs[0])
    both(params_wait, range(6))
    norm_stage(0)
    for i, pair in enumerate(group_pairs):
        both(add_first, pair)
        if i == 0:
            norm_stage(1)
    norm_stage(2)
    for pair in group_pairs:
        both(update, pair)
    norm_stage(3)
    for pair in group_pairs:
        both(spread, pair)
    for act in (pass_on, finish):
        for pair in in_pairs:
            both(act, pair)
    both(sent, range(6))


def write_out(shapes, n, *refs):
    refs = list(refs)

    def take(count):
        out, refs[:] = refs[:count], refs[count:]
        return out

    gathered, news, states, norms = take(6), take(6), take(6), take(3)
    copies, new_outs, state_outs, norm_outs = take(6), take(6), take(6), take(3)
    sems, norm_sems = take(2)
    for m in range(6):
        if BY_ROWS[m]:
            pltpu.make_async_copy(gathered[m], copies[m], sems.at[m, 0]).start()
        else:
            width = shapes[m][1]
            for j in range(n):
                source = gathered[m].at[j // 4, j // 2 % 2, j % 2]
                target = copies[m].at[:, pl.ds(j * width, width)]
                pltpu.make_async_copy(source, target, sems.at[m, 0]).start()
        pltpu.make_async_copy(news[m], new_outs[m], sems.at[m, 1]).start()
        pltpu.make_async_copy(states[m], state_outs[m], sems.at[m, 1]).start()
    moves = [
        pltpu.make_async_copy(a, b, norm_sems.at[i])
        for i, (a, b) in enumerate(zip(norms, norm_outs))
    ]
    for move in moves:
        move.start()
    for m in range(6):
        every, half = gathered[m], gathered[m].at[0]
        pltpu.make_async_copy(every, every, sems.at[m, 0]).wait()
        pltpu.make_async_copy(half, half, sems.at[m, 1]).wait()
    for move in moves:
        move.wait()


def kernel_body(*args):
    n = lax.axis_size("batch")
    grads, grad_norm = [a[0] for a in args[:6]], args[6]
    weights, weight_norm = args[7:13], args[13]
    moments, moment_norm = args[14:20], args[20]
    shapes = [w.shape for w in weights]
    grads = [g.reshape((n, *s)) if by_rows else g for g, s, by_rows in zip(grads, shapes, BY_ROWS)]
    width = weight_norm.shape[0]
    bf16, f32 = jnp.bfloat16, jnp.float32
    any_spec = pl.BlockSpec(memory_space=pl.ANY)
    vmem_spec = pl.BlockSpec(memory_space=pltpu.VMEM)
    hbm_spec = pl.BlockSpec(memory_space=pltpu.HBM)
    lists = pieces_of(shapes)
    groups = [group for pair in zip(*lists) for group in pair]
    pieces = [piece for groups_s in lists for group in groups_s for piece in group[-1]]
    assert len(groups) == 2 * len(lists[0]) and len(groups) == 2 * len(lists[1])

    def scratch(parts, lead, kind):
        return [pltpu.VMEM((*lead, part[3], shapes[part[1]][1]), kind) for part in parts]

    plain = [jax.ShapeDtypeStruct(s, f32) for s in shapes] * 2 + [
        jax.ShapeDtypeStruct((n, width), bf16),
        jax.ShapeDtypeStruct((1, width), f32),
        jax.ShapeDtypeStruct((1, width), f32),
    ]
    parts = [jax.ShapeDtypeStruct((2, 2, 2, *s), bf16) for s in shapes]
    norms = (grad_norm, weight_norm.reshape(1, width), moment_norm.reshape(1, width))
    arrays = (*grads, *weights, *moments, *norms)
    results = pl.pallas_call(
        functools.partial(exchange, shapes, n),
        out_shape=parts + plain,
        in_specs=[any_spec] * 21,
        out_specs=[vmem_spec] * 21,
        scratch_shapes=[pltpu.VMEM(g.shape, f32) for g in grads]
        + [pltpu.VMEM((2, *s), f32) for s in shapes]
        + scratch(pieces, (4,), bf16) * 2
        + scratch(pieces, (2,), bf16) * 2
        + scratch(pieces, (2,), f32)
        + scratch(groups, (), bf16) * 2
        + scratch(groups, (), f32)
        + [pltpu.VMEM((1, n * width), f32)]
        + [pltpu.VMEM((1, width), f32)] * 2
        + [pltpu.VMEM((3, 3, n, width), f32)] * 2
        + [pltpu.VMEM((2, n, width), f32)]
        + [
            pltpu.SemaphoreType.DMA((len(pieces), KINDS)),
            pltpu.SemaphoreType.DMA((6,)),
            pltpu.SemaphoreType.DMA((len(groups),)),
            pltpu.SemaphoreType.DMA((4,)),
            pltpu.SemaphoreType.DMA((2,)),
        ],
        compiler_params=pltpu.CompilerParams(
            collective_id=0, has_side_effects=True, vmem_limit_bytes=40 * 2**20
        ),
    )(*[pltpu.with_memory_space_constraint(a, pltpu.HBM) for a in arrays])
    finals = pl.pallas_call(
        functools.partial(write_out, shapes, n),
        out_shape=[
            part if by_rows else jax.ShapeDtypeStruct((s[0], n * s[1]), bf16)
            for part, s, by_rows in zip(parts, shapes, BY_ROWS)
        ]
        + plain,
        in_specs=[any_spec] * 21,
        out_specs=[hbm_spec] * 21,
        scratch_shapes=[pltpu.SemaphoreType.DMA((6, 2)), pltpu.SemaphoreType.DMA((3,))],
        compiler_params=pltpu.CompilerParams(vmem_limit_bytes=8 * 2**20),
    )(*[pltpu.with_memory_space_constraint(r, pltpu.VMEM) for r in results])
    copy = [f.reshape(-1, f.shape[-1]) for f in finals[:6]]
    new, state = finals[6:12], finals[12:18]
    copy_norm, new_norm, state_norm = (r.reshape(-1) for r in finals[18:])
    return (*copy, copy_norm, *new, new_norm, *state, state_norm)


def chosen(*args):
    fits = lax.axis_size("batch") == 2**3 and args[13].shape[0] % 128 == 0
    for m, shares in PLANS[0] + PLANS[1]:
        w = args[7 + m]
        fits = fits and w.shape[0] % (16 * sum(map(sum, shares))) == 0 and w.shape[1] % 128 == 0
    return kernel_body(*args) if fits else body(*args)


def solution(mesh):
    in_specs = (
        P("batch", None, "cols"),
        P("batch", "cols", None),
        P("batch", None, "cols"),
        P("batch", None, "cols"),
        P("batch", None, "cols"),
        P("batch", "cols", None),
        P("batch", None),
        P("batch", "cols"),
        P("cols", "batch"),
        P("batch", "cols"),
        P("batch", "cols"),
        P("batch", "cols"),
        P("cols", "batch"),
        P("batch"),
        P("batch", "cols"),
        P("cols", "batch"),
        P("batch", "cols"),
        P("batch", "cols"),
        P("batch", "cols"),
        P("cols", "batch"),
        P("batch"),
    )
    out_specs = (
        P(None, "cols"),
        P("cols", None),
        P(None, "cols"),
        P(None, "cols"),
        P(None, "cols"),
        P("cols", None),
        P(),
        P("batch", "cols"),
        P("cols", "batch"),
        P("batch", "cols"),
        P("batch", "cols"),
        P("batch", "cols"),
        P("cols", "batch"),
        P("batch"),
        P("batch", "cols"),
        P("cols", "batch"),
        P("batch", "cols"),
        P("batch", "cols"),
        P("batch", "cols"),
        P("cols", "batch"),
        P("batch"),
    )
    return jax.shard_map(chosen, mesh=mesh, in_specs=in_specs, out_specs=out_specs, check_vma=False)
```
